256 devices in a mesh: seq: 256 (over x, y, z, core).
Axes of the slice: x: 4, y: 4, z: 8, core: 2. Of those that a mesh axis runs over, the one named last changes fastest.
Arguments:
- history: float32 [98304, 1024], P('seq'), may hold values from -6 to 6
- taps: float32 [98304, 1024], P('seq'), may hold values from -0.078125 to 0.078125
- self_taps: float32 [1024, 256], P('seq'), may hold values from -0.375 to 0.375
- fresh: float32 [1024, 256], P('seq'), may hold values from -6 to 6
- gate: float32 [1024, 256], P('seq'), may hold values from -6 to 6
Outputs:
- gated: float32 [1024, 256], P('seq')
The draws below stay inside these ranges and needn't reach their ends.
All inputs are finite; a program needn't handle non-finite values.
Results may differ from the reference program's by a relative error of at most 0.000053.
Values sent between devices are 32-bit elements; how exact they have to be, the bound alone decides.
A program may use at most 64 MiB of HBM per device.

```python
import jax
import jax.numpy as jnp
from jax import lax

CHANNELS = 1024
NEW_TOKENS = 256
HISTORY = 98304


def raised(entries, key, source, target, shards_of, factor):
    owner, partner = [(jnp.arange(entries.shape[dim]) // (entries.shape[dim] // shards_of)).reshape([-1 if axis == dim else 1 for axis in range(entries.ndim)]) for dim in (source, target)]
    chosen = jax.random.permutation(key, shards_of)[partner]
    strong = (owner == chosen) | (owner == (partner + shards_of // 2) % shards_of)
    return jnp.where(strong, factor * entries, entries)


def steps_of(own_key, shape, shards, smallest, high):
    gain, own = 1.0, jax.random.fold_in(own_key, 6)
    for dim, shards_of in shards:
        heights = jnp.exp(jax.random.uniform(jax.random.fold_in(own, dim), (shards_of,), jnp.float32, smallest / len(shards), high / len(shards)))
        gain = gain * jnp.repeat(heights, shape[dim] // shards_of).reshape([-1 if axis == dim else 1 for axis in range(len(shape))])
    return gain


def gaussian(rng, shape, deviation, reach, split=(), dtype=jnp.bfloat16):
    level = steps_of(rng, shape, split, -0.22, 0.18) if split else 1.0
    entries = jax.random.normal(rng, shape, jnp.float32) * deviation * level
    return jnp.minimum(jnp.maximum(entries, -reach), reach).astype(dtype)


def heavy_noise(own_key, shape, spread, most, split, heavy, held_as=jnp.bfloat16):
    array = spread * jax.random.normal(own_key, shape, jnp.float32)
    if split:
        array = array * steps_of(own_key, shape, split, -0.22, 0.18)
    return jnp.clip(raised(array, jax.random.fold_in(own_key, 3), *heavy), -most, most).astype(held_as)


def setup_inputs(seed: int = 0) -> dict:
    arg_keys = jax.random.split(jax.random.key(seed), 6)
    return {
        "history": gaussian(arg_keys[0], (HISTORY, CHANNELS), 1.0, 6.0, ((0, 256),), jnp.float32),
        "taps": heavy_noise(arg_keys[1], (HISTORY, CHANNELS), HISTORY ** -0.5, 0.078125, ((0, 256),), (0, 1, 256, 6.0), jnp.float32),
        "self_taps": gaussian(arg_keys[2], (CHANNELS, NEW_TOKENS), NEW_TOKENS ** -0.5, 0.375, ((0, 256),), jnp.float32),
        "fresh": gaussian(arg_keys[3], (CHANNELS, NEW_TOKENS), 1.0, 6.0, ((0, 256),), jnp.float32),
        "gate": gaussian(arg_keys[4], (CHANNELS, NEW_TOKENS), 1.0, 6.0, ((0, 256),), jnp.float32),
    }


def correlate(pair):
    hist_block, taps_block = pair
    length = 2 * HISTORY
    hist_spec = jnp.fft.rfft(hist_block, n=length, axis=0)
    taps_spec = jnp.fft.rfft(taps_block, n=length, axis=0)
    return jnp.fft.irfft(jnp.conj(taps_spec) * hist_spec, n=length, axis=0)[:NEW_TOKENS]


def reference(history, taps, self_taps, fresh, gate):
    groups = CHANNELS // 32
    hist_blocks = history.reshape(HISTORY, groups, 32).transpose(1, 0, 2)
    taps_blocks = taps.reshape(HISTORY, groups, 32).transpose(1, 0, 2)
    lagged = lax.map(correlate, (hist_blocks, taps_blocks))
    hist_part = lagged.transpose(0, 2, 1).reshape(CHANNELS, NEW_TOKENS)
    doubled = 2 * NEW_TOKENS
    own_spec = jnp.fft.rfft(self_taps, n=doubled, axis=1) * jnp.fft.rfft(fresh, n=doubled, axis=1)
    own_part = jnp.fft.irfft(own_spec, n=doubled, axis=1)[:, :NEW_TOKENS]
    return gate * (hist_part + own_part)
```

```python
import functools
import math

import jax
import jax.numpy as jnp
import numpy as np
from jax import lax
from jax.experimental import pallas as pl
from jax.experimental.pallas import tpu as pltpu
from jax.sharding import PartitionSpec as P

MESH = pl.DeviceIdType.MESH
F32 = jnp.float32
BF16 = jnp.bfloat16
NX, NY, NZ = 4, 4, 8
B = 128
L2 = 2 * B
TILES = 8


def split_pair(matrix):
    high = matrix.astype(jnp.bfloat16)
    low = (matrix - high.astype(np.float64)).astype(jnp.bfloat16)
    return high, low


def tables():
    j = np.concatenate([np.arange(0, B, 2), np.arange(1, B, 2)])
    angle = 2.0 * math.pi / L2 * np.outer(j + 0.5, np.arange(B))
    forward = np.concatenate([np.cos(angle), -np.sin(angle)], axis=0)
    inverse = np.concatenate([np.cos(angle), np.sin(angle)], axis=0).T / B
    f_high, f_low = split_pair(forward)
    g_high, g_low = split_pair(inverse)
    both = np.concatenate(
        [np.concatenate([f_high, f_high], axis=1), np.concatenate([f_low, f_low], axis=1)], axis=0
    )
    return both, np.concatenate([g_high, g_low], axis=0)


def halves(value):
    high = value.astype(BF16)
    low = (value - high.astype(F32)).astype(BF16)
    return high, low


def kernel(
    history, taps, self_taps, fresh, gate, f_in, g_in, out_ref,
    h_buf, t_buf, prev_t, next_h, f_buf, g_buf, small, spec, acc0, acc1, keep, own_buf,
    y_buf, rc_buf, z_buf, r1_buf, u_buf, r2_buf, v_buf, r3_buf,
    load_sem, const_sem, nf_send, nf_recv, nb_send, nb_recv, c_send, c_recv,
    s1_send, s1_recv, s2_send, s2_recv, s3_send, s3_recv,
):
    me = lax.axis_index("seq")
    last = NX * NY * NZ * 2 - 1
    core = me % 2
    z = (me // 2) % NZ
    y = (me // (2 * NZ)) % NY
    x = me // (2 * NZ * NY)

    def device(dx, dy, dz, dc):
        return ((dx * NY + dy) * NZ + dz) * 2 + dc

    partner = device(x, y, z, 1 - core)

    barrier = pltpu.get_barrier_semaphore()

    def greet(target):
        pl.semaphore_signal(barrier, inc=1, device_id=(target,), device_id_type=MESH)

    for step in (4, 3, 5, 2, 6, 1, 7):
        for side in (0, 1):
            greet(device(x, y, (z + step) % NZ, side))
    for step in (2, 1, 3):
        greet(device((x + step) % NX, y, z, core))
        greet(device(x, (y + step) % NY, z, core))
    pl.when(me > 0)(lambda: greet(me - 1))
    pl.when(me < last)(lambda: greet(me + 1))
    greet(partner)

    def tile_of(n, dev):
        tx = dev // (2 * NZ * NY)
        ty = (dev // (2 * NZ)) % NY
        odd = ty // 2
        return 2 * ((tx + 1 + n % 4) % 4) + (odd + 1 + n // 4) % 2

    def load(n, go):
        tile = tile_of(n, me)
        lanes = pl.ds(pl.multiple_of(tile * B, B), B)
        for which, (source, target) in enumerate(((history, h_buf), (taps, t_buf))):
            go(pltpu.make_async_copy(source.at[:, lanes], target.at[tile], load_sem.at[tile, which]))

    consts = [
        pltpu.make_async_copy(f_in, f_buf, const_sem.at[0]),
        pltpu.make_async_copy(g_in, g_buf, const_sem.at[1]),
        pltpu.make_async_copy(self_taps, small.at[0], const_sem.at[2]),
        pltpu.make_async_copy(fresh, small.at[1], const_sem.at[3]),
        pltpu.make_async_copy(gate, small.at[2], const_sem.at[4]),
    ]
    consts[0].start()

    def start_load(n, _):
        load(n, lambda copy: copy.start())
        return 0

    lax.fori_loop(0, TILES, start_load, 0)
    for copy in consts[1:]:
        copy.start()
    consts[0].wait()

    def transform(blocks):
        pairs = [halves(block) for block in blocks]
        weights = jnp.concatenate(
            [
                jnp.concatenate([pair[0] for pair in pairs], axis=1),
                jnp.concatenate([pair[1] for pair in pairs], axis=1),
            ],
            axis=0,
        )
        result = jnp.dot(f_buf[...], weights, preferred_element_type=F32)
        return result[:L2] + result[L2:]

    ROWS = 16

    def chunks():
        for start in range(0, B, ROWS):
            yield slice(start, start + ROWS), slice(B + start, B + start + ROWS), start < B // 2

    def turned(real, imag, even):
        return (-imag, real) if even else (imag, -real)

    def times(a, h):
        return a[0] * h[0] + a[1] * h[1], a[1] * h[0] - a[0] * h[1]

    def total(*terms):
        real, imag = terms[0]
        for term in terms[1:]:
            real, imag = real + term[0], imag + term[1]
        return real, imag

    def own_spectra(n, _):
        tile = tile_of(n, me)
        for pair in range(3):
            rows = pl.ds(pair * B, B)
            spec[pair] = transform([h_buf[tile, rows, :], t_buf[tile, rows, :]])
        for re, im, even in chunks():
            h = [(spec[k, re, :B], spec[k, im, :B]) for k in range(3)]
            t = [(spec[k, re, B:], spec[k, im, B:]) for k in range(3)]
            w1 = total(t[1], turned(*t[0], even))
            w2 = total(t[2], turned(*t[1], even))
            s0 = total(times(t[0], h[0]), times(w1, h[1]), times(w2, h[2]))
            s1 = total(times(t[0], h[1]), times(w1, h[2]))
            for rows, part in ((re, 0), (im, 1)):
                acc0[tile, rows, :] = s0[part]
                acc1[tile, rows, :] = s1[part]
                keep[tile, 0, rows, :] = h[0][part]
                keep[tile, 1, rows, :] = h[1][part]
                keep[tile, 2, rows, :] = t[1][part]
        return 0

    def forward_copy(tile):
        return pltpu.make_async_remote_copy(
            src_ref=t_buf.at[tile, pl.ds(2 * B, B)], dst_ref=prev_t.at[tile],
            send_sem=nf_send.at[tile], recv_sem=nf_recv.at[tile],
            device_id=(me + 1,), device_id_type=MESH,
        )

    def backward_copy(tile):
        return pltpu.make_async_remote_copy(
            src_ref=h_buf.at[tile, pl.ds(0, B)], dst_ref=next_h.at[tile],
            send_sem=nb_send.at[tile], recv_sem=nb_recv.at[tile],
            device_id=(me - 1,), device_id_type=MESH,
        )

    load(0, lambda copy: copy.wait())
    own_spectra(0, 0)
    pl.semaphore_wait(
        barrier, 21 + jnp.where(me > 0, 1, 0) + jnp.where(me < last, 1, 0)
    )

    def wait_load(n, _):
        load(n, lambda copy: copy.wait())
        return 0

    def start_neighbours(n, _):
        @pl.when(me < last)
        def _():
            forward_copy(tile_of(n, me + 1)).start()

        @pl.when(me > 0)
        def _():
            backward_copy(tile_of(n, me - 1)).start()

        return 0

    lax.fori_loop(1, TILES, wait_load, 0)
    lax.fori_loop(0, TILES, start_neighbours, 0)

    @pl.when(me == 0)
    def _():
        prev_t[...] = jnp.zeros_like(prev_t)

    @pl.when(me == last)
    def _():
        next_h[...] = jnp.zeros_like(next_h)

    lax.fori_loop(1, TILES, own_spectra, 0)

    for copy in consts[1:]:
        copy.wait()
    row = lax.broadcasted_iota(jnp.int32, (L2, L2), 0)
    column = lax.broadcasted_iota(jnp.int32, (L2, L2), 1)
    late = column >= row
    fresh_columns = jnp.concatenate([small[1], jnp.zeros((4, L2), F32)], axis=0).T
    for c in range(4):
        filters = jnp.broadcast_to(small[0, c : c + 1, :], (L2, L2))
        shifted = pltpu.roll(filters, 0, 1, stride=1, stride_axis=0)
        products = jnp.where(late, shifted, 0.0) * fresh_columns[:, c : c + 1]
        own_buf[c : c + 1, :] = products.sum(axis=0, keepdims=True)

    mine1 = jnp.where(core == 0, x, y)
    mine2 = jnp.where(core == 0, y, x)

    def core_copy(tile):
        return pltpu.make_async_remote_copy(
            src_ref=y_buf.at[1 - core, tile], dst_ref=rc_buf.at[tile],
            send_sem=c_send.at[tile], recv_sem=c_recv.at[tile],
            device_id=(partner,), device_id_type=MESH,
        )

    def half_index(p, o):
        return jnp.where(core == 0, p * 4 + o, o * 4 + p)

    def stage1_copy(p, o):
        target = device(jnp.where(core == 0, p, x), jnp.where(core == 0, y, p), z, core)
        return pltpu.make_async_remote_copy(
            src_ref=z_buf.at[half_index(p, o)], dst_ref=r1_buf.at[mine1, o],
            send_sem=s1_send.at[p, o], recv_sem=s1_recv.at[mine1, o],
            device_id=(target,), device_id_type=MESH,
        )

    def stage1_arrival(source, o):
        return pltpu.make_async_remote_copy(
            src_ref=z_buf.at[0], dst_ref=r1_buf.at[source, o],
            send_sem=s1_send.at[source, o], recv_sem=s1_recv.at[source, o],
            device_id=(partner,), device_id_type=MESH,
        )

    def stage2_copy(o):
        target = device(jnp.where(core == 0, x, o), jnp.where(core == 0, o, y), z, core)
        return pltpu.make_async_remote_copy(
            src_ref=u_buf.at[o], dst_ref=r2_buf.at[mine2],
            send_sem=s2_send.at[o], recv_sem=s2_recv.at[mine2],
            device_id=(target,), device_id_type=MESH,
        )

    def stage2_arrival(source):
        return pltpu.make_async_remote_copy(
            src_ref=u_buf.at[0], dst_ref=r2_buf.at[source],
            send_sem=s2_send.at[source], recv_sem=s2_recv.at[source],
            device_id=(partner,), device_id_type=MESH,
        )

    def stage3_copy(tz, tc):
        return pltpu.make_async_remote_copy(
            src_ref=v_buf.at[tz], dst_ref=r3_buf.at[z, core],
            send_sem=s3_send.at[tz, tc], recv_sem=s3_recv.at[z, core],
            device_id=(device(x, y, tz, tc),), device_id_type=MESH,
        )

    def stage3_arrival(sz, sc):
        return pltpu.make_async_remote_copy(
            src_ref=v_buf.at[0], dst_ref=r3_buf.at[sz, sc],
            send_sem=s3_send.at[sz, sc], recv_sem=s3_recv.at[sz, sc],
            device_id=(partner,), device_id_type=MESH,
        )

    def halves_of(tile):
        for b in range(2):
            first, second = tile // 2, 2 * (tile % 2) + b
            yield jnp.where(core == 0, first, second), jnp.where(core == 0, second, first)

    def pass_on(n):
        tile = tile_of(n, me)
        core_copy(tile).wait_recv()
        for b in range(2):
            rows = pl.ds(b * 64, 64)
            z_buf[2 * tile + b] = y_buf[core, tile, rows, :] + rc_buf[tile, rows, :]
        for p, o in halves_of(tile):
            @pl.when(p != mine1)
            def _():
                stage1_copy(p, o).start()

    def finish(n, _):
        tile = tile_of(n, me)

        @pl.when(me > 0)
        def _():
            forward_copy(tile).wait_recv()

        @pl.when(me < last)
        def _():
            backward_copy(tile).wait_recv()

        spec[0] = transform([next_h[tile], prev_t[tile]])
        for re, im, even in chunks():
            h3 = (spec[0, re, :B], spec[0, im, :B])
            q = (spec[0, re, B:], spec[0, im, B:])
            h0 = (keep[tile, 0, re, :], keep[tile, 0, im, :])
            h1 = (keep[tile, 1, re, :], keep[tile, 1, im, :])
            t1 = turned(keep[tile, 2, re, :], keep[tile, 2, im, :], even)
            v = turned(*q, even)
            a0 = (acc0[tile, re, :], acc0[tile, im, :])
            a1 = (acc1[tile, re, :], acc1[tile, im, :])
            s0 = total(a0, times(v, h0))
            s1 = total(a1, times(q, h0), times(v, h1), times(t1, h3))
            for rows, part in ((re, 0), (im, 1)):
                spec[1, rows, :B] = s0[part]
                spec[1, rows, B:] = s1[part]
        high, low = halves(spec[1])
        main = jnp.dot(g_buf[...], high, preferred_element_type=F32)
        rest = jnp.dot(g_buf[:B], low, preferred_element_type=F32)
        lagged = main[:B] + (main[B:] + rest)
        for q in range(2):
            y_buf[q, tile] = lagged[:, q * B : (q + 1) * B].T
        core_copy(tile).start()

        @pl.when(n > 0)
        def _():
            pass_on(n - 1)

        return 0

    lax.fori_loop(0, TILES, finish, 0)
    pass_on(TILES - 1)

    def add_first(i, _):
        o = (mine2 + 1 + i) % 4
        value = z_buf[half_index(mine1, o)]
        for k in range(1, 4):
            source = (mine1 + k) % 4
            stage1_arrival(source, o).wait_recv()
            value = value + r1_buf[source, o]
        u_buf[o] = value

        @pl.when(i < 3)
        def _():
            stage2_copy(o).start()

        return 0

    lax.fori_loop(0, 4, add_first, 0)
    value = u_buf[mine2]
    for k in range(1, 4):
        source = (mine2 + k) % 4
        stage2_arrival(source).wait_recv()
        value = value + r2_buf[source]
    v_buf[...] = value.reshape(NZ, 8, B)
    for step in (4, 3, 5, 2, 6, 1, 7):
        for side in (0, 1):
            stage3_copy((z + step) % NZ, side).start()
    stage3_copy(z, 1 - core).start()
    r3_buf[z, core] = v_buf[z]

    stage3_arrival(z, 1 - core).wait_recv()
    for step in range(1, NZ):
        for side in (0, 1):
            stage3_arrival((z + step) % NZ, side).wait_recv()
    parts = []
    for side in (0, 1):
        part = r3_buf[0, side]
        for k in range(1, NZ):
            part = part + r3_buf[k, side]
        parts.append(part)
    summed = jnp.concatenate(parts, axis=1)
    hist_part = jnp.where(core == 0, summed[:4], summed[4:])
    out_ref[...] = small[2] * (hist_part + own_buf[...])

    def drain(n, _):
        tile = tile_of(n, me)

        @pl.when(me < last)
        def _():
            forward_copy(tile).wait_send()

        @pl.when(me > 0)
        def _():
            backward_copy(tile).wait_send()

        core_copy(tile).wait_send()
        for p, o in halves_of(tile):
            @pl.when(p != mine1)
            def _():
                stage1_copy(p, o).wait_send()

        return 0

    lax.fori_loop(0, TILES, drain, 0)
    for k in range(1, 4):
        stage2_copy((mine2 + k) % 4).wait_send()
    stage3_copy(z, 1 - core).wait_send()
    for step in range(1, NZ):
        for side in (0, 1):
            stage3_copy((z + step) % NZ, side).wait_send()


def body(history, taps, self_taps, fresh, gate):
    f_table, g_table = (jnp.asarray(table) for table in tables())
    anywhere = pl.BlockSpec(memory_space=pl.ANY)
    dma = pltpu.SemaphoreType.DMA
    return pl.pallas_call(
        kernel,
        out_shape=jax.ShapeDtypeStruct((4, 256), F32),
        in_specs=[anywhere] * 7,
        out_specs=pl.BlockSpec(memory_space=pltpu.VMEM),
        scratch_shapes=[
            pltpu.VMEM((TILES, 384, B), F32),
            pltpu.VMEM((TILES, 384, B), F32),
            pltpu.VMEM((TILES, B, B), F32),
            pltpu.VMEM((TILES, B, B), F32),
            pltpu.VMEM((512, 256), BF16),
            pltpu.VMEM((256, 256), BF16),
            pltpu.VMEM((3, 4, 256), F32),
            pltpu.VMEM((3, L2, L2), F32),
            pltpu.VMEM((TILES, L2, B), F32),
            pltpu.VMEM((TILES, L2, B), F32),
            pltpu.VMEM((TILES, 3, L2, B), F32),
            pltpu.VMEM((4, 256), F32),
            pltpu.VMEM((2, TILES, B, B), F32),
            pltpu.VMEM((TILES, B, B), F32),
            pltpu.VMEM((16, 64, B), F32),
            pltpu.VMEM((4, 4, 64, B), F32),
            pltpu.VMEM((4, 64, B), F32),
            pltpu.VMEM((4, 64, B), F32),
            pltpu.VMEM((NZ, 8, B), F32),
            pltpu.VMEM((NZ, 2, 8, B), F32),
            dma((TILES, 2)),
            dma((5,)),
            dma((TILES,)),
            dma((TILES,)),
            dma((TILES,)),
            dma((TILES,)),
            dma((TILES,)),
            dma((TILES,)),
            dma((4, 4)),
            dma((4, 4)),
            dma((4,)),
            dma((4,)),
            dma((NZ, 2)),
            dma((NZ, 2)),
        ],
        compiler_params=pltpu.CompilerParams(
            collective_id=0, has_side_effects=True, vmem_limit_bytes=48 * 1024 * 1024
        ),
    )(history, taps, self_taps, fresh, gate, f_table, g_table)


def solution(mesh):
    spec = P("seq", None)
    return jax.shard_map(
        body, mesh=mesh, in_specs=(spec,) * 5, out_specs=spec, check_vma=False
    )
```
